32 devices in a mesh: occ: 8 (over z, y), ao: 4 (over x, core).
Axes of the slice: x: 2, y: 2, z: 4, core: 2. Of those that a mesh axis runs over, the one named last changes fastest.
Arguments:
- amplitudes: bfloat16 [8, 640, 19456], P(None, 'occ', 'ao'), may hold values from -6 to 6
- occ_coef: bfloat16 [512, 640], P(None, 'occ'), may hold values from -0.25 to 0.25
- vir_coef: bfloat16 [512, 19456], P('occ', 'ao'), may hold values from -0.25 to 0.25
- occ_energy: float32 [640], P('occ'), may hold values from -1.5 to -0.3
- vir_energy: float32 [19456], P('ao'), may hold values from 0.05 to 2.5
- kernel: float32 [512], replicated, may hold values from 2 to 10
Outputs:
- residual: bfloat16 [8, 640, 19456], P(None, 'occ', 'ao')
- projected: float32 [8, 8], replicated
The draws below stay inside these ranges and needn't reach their ends.
All inputs are finite; a program needn't handle non-finite values.
Results may differ from the reference program's by a relative error of at most 0.0049.
Values may be sent and summed in bfloat16 or wider, within the bound.
A program may use at most 128 MiB of HBM per device.

```python
import math
import jax
import jax.numpy as jnp
from jax import lax

K = 8
NVIR = 19456
ROWS = 512
NOCC = 640


def level_of(own_key, shape, cuts, smallest, high):
    factor_of, own = 1.0, jax.random.fold_in(own_key, 6)
    for position, shards_of in cuts:
        draws = jnp.exp(jax.random.uniform(jax.random.fold_in(own, position), (shards_of,), jnp.float32, smallest / len(cuts), high / len(cuts)))
        factor_of = factor_of * jnp.repeat(draws, shape[position] // shards_of).reshape([-1 if axis == position else 1 for axis in range(len(shape))])
    return factor_of


def bell_draw(key, shape, deviation, limit, pieces=(), dtype=jnp.bfloat16):
    array = jax.random.normal(key, shape, jnp.float32) * deviation
    if len(pieces) > 0:
        array = level_of(key, shape, pieces, -0.22, 0.18) * array
    return jnp.clip(array, min=-limit, max=limit).astype(dtype)


def setup_inputs(seed: int = 0) -> dict:
    splits = jax.random.split(jax.random.key(seed), 7)
    amplitudes = bell_draw(splits[0], (K, NOCC, NVIR), 1.0, 6.0, ((1, 8), (2, 4)))
    occ_coef = bell_draw(splits[1], (ROWS, NOCC), ROWS ** -0.5, 0.25, ((1, 8),))
    vir_coef = bell_draw(splits[2], (ROWS, NVIR), ROWS ** -0.5, 0.25, ((0, 8), (1, 4)))
    occ_energy = jnp.clip(-1.5 + 1.2 * jax.random.uniform(splits[3], (NOCC,), jnp.float32) ** level_of(splits[3], (NOCC,), ((0, 8),), -0.2, 0.2), -1.5, -0.3)
    vir_energy = jnp.clip(0.05 + 2.45 * jax.random.uniform(splits[4], (NVIR,), jnp.float32) ** level_of(splits[4], (NVIR,), ((0, 4),), -0.2, 0.2), 0.05, 2.5)
    kernel = jnp.clip(jnp.exp(jax.random.uniform(splits[5], (ROWS,), jnp.float32, math.log(2.0), math.log(10.0))), 2.0, 10.0)
    return {"amplitudes": amplitudes, "occ_coef": occ_coef, "vir_coef": vir_coef, "occ_energy": occ_energy, "vir_energy": vir_energy, "kernel": kernel}


def reference(amplitudes, occ_coef, vir_coef, occ_energy, vir_energy, kernel):
    occ_float = occ_coef.astype(jnp.float32)
    energy_gaps = vir_energy[None, :] - occ_energy[:, None]

    def sigma_of(trial_amps):
        half_done = jnp.dot(trial_amps, vir_coef.T, preferred_element_type=jnp.float32)
        density = lax.optimization_barrier(jnp.sum(occ_float.T * half_done, axis=0))
        potential = kernel * density
        weighted = (occ_float * potential[:, None]).astype(jnp.bfloat16)
        coupling = jnp.dot(weighted.T, vir_coef, preferred_element_type=jnp.float32)
        return energy_gaps * trial_amps.astype(jnp.float32) + coupling
    sigma_all = lax.map(sigma_of, amplitudes)
    flat_amps = amplitudes.reshape(K, -1)
    correlation = jnp.dot(flat_amps, flat_amps.T, preferred_element_type=jnp.float32)

    def gram_column(sigma_one):

        def one_entry(trial_amps):
            return jnp.sum(trial_amps.astype(jnp.float32) * sigma_one)
        return lax.map(one_entry, amplitudes)
    gram = lax.map(gram_column, sigma_all).T
    norms = jnp.diagonal(correlation) + 1e-06
    ritz_values = jnp.diagonal(gram) / norms
    residual = (sigma_all - ritz_values[:, None, None] * amplitudes.astype(jnp.float32)).astype(jnp.bfloat16)
    projected = gram / jnp.sqrt(norms[:, None] * norms[None, :])
    return (residual, projected)
```

```python
import functools

import jax
import jax.numpy as jnp
from jax import lax
from jax.experimental import pallas as pl
from jax.experimental.pallas import tpu as pltpu
from jax.sharding import PartitionSpec as P

LANES = 128
MESH = pl.DeviceIdType.MESH
F32 = jnp.float32


def split_tiles(first, last, parts):
    parts = min(parts, last - first)
    runs, at = [], first
    for j in range(parts):
        size = (last - at) // (parts - j)
        size += 1 if (last - at) % (parts - j) else 0
        runs.append((at * LANES, size * LANES))
        at += size
    return runs


def exchange(box, me, size, axis, send, recv):
    copies = []
    for d in range(1, size):
        copy = pltpu.make_async_remote_copy(
            src_ref=box.at[me],
            dst_ref=box.at[me],
            send_sem=send.at[d - 1],
            recv_sem=recv.at[me],
            device_id={axis: lax.rem(me + d, size)},
            device_id_type=MESH,
        )
        copy.start()
        copies.append(copy)
    for d in range(1, size):
        other = lax.rem(me + d, size)
        pltpu.make_async_remote_copy(
            src_ref=box.at[other],
            dst_ref=box.at[other],
            send_sem=send.at[d - 1],
            recv_sem=recv.at[other],
            device_id={axis: other},
            device_id_type=MESH,
        ).wait_recv()
    for copy in copies:
        copy.wait_send()


def gather_kernel(
    n,
    m,
    trials,
    runs,
    amps_hbm,
    vir_hbm,
    occ_ref,
    occ_energy_ref,
    vir_energy_ref,
    rows_hbm,
    stats_ref,
    amps,
    rows,
    dens,
    acc,
    box_ao,
    box_occ,
    local_sem,
    send_sem,
    recv_sem,
    ao_send,
    ao_recv,
    occ_send,
    occ_recv,
):
    own, col = lax.axis_index("occ"), lax.axis_index("ao")
    occ_dev = amps.shape[0] // trials
    tiles = amps.shape[1] // LANES
    total = n * rows.shape[1]
    pieces = len(runs[0])

    def place(p):
        back = p // (n // 2)
        return (1 - back) * 2 * p + back * (2 * (n - 1 - p) + 1)

    parity, half = lax.rem(own, 2), own // 2
    spot = parity * (n - 1 - half) + (1 - parity) * half
    toward = (place(lax.rem(spot + 1, n)), place(lax.rem(spot + n - 1, n)))

    take_rows = pltpu.make_async_copy(vir_hbm, rows.at[own], local_sem.at[0])
    take_rows.start()
    take_amps = pltpu.make_async_copy(amps_hbm, amps, local_sem.at[1])
    take_amps.start()

    barrier = pltpu.get_barrier_semaphore()
    for d in range(1, n):
        pl.semaphore_signal(
            barrier, inc=1, device_id={"occ": lax.rem(own + d, n)}, device_id_type=MESH
        )
    for d in range(1, m):
        pl.semaphore_signal(
            barrier, inc=1, device_id={"ao": lax.rem(col + d, m)}, device_id_type=MESH
        )
    pl.semaphore_wait(barrier, n + m - 2)
    take_rows.wait()

    def slot_of(way, age):
        if way == 0:
            return place(lax.rem(spot - age + n, n))
        return place(lax.rem(spot + age, n))

    def hop(way, j, slot, step):
        start, width = runs[way][j]
        piece = rows.at[slot, :, pl.ds(start, width)]
        return pltpu.make_async_remote_copy(
            src_ref=piece,
            dst_ref=piece,
            send_sem=send_sem.at[way, j, lax.rem(step, 2)],
            recv_sem=recv_sem.at[way, j, step],
            device_id={"occ": toward[way]},
            device_id_type=MESH,
        )

    def contract(way, j, slot):
        start, width = runs[way][j]
        half_done = lax.dot_general(
            amps[:, pl.ds(start, width)],
            rows[slot, :, pl.ds(start, width)],
            (((1,), (1,)), ((), ())),
            preferred_element_type=F32,
        )
        half_done = half_done.reshape(trials, occ_dev, rows.shape[1])
        dens[slot] += jnp.sum(half_done * occ_ref[slot][None], axis=1)

    pairs = [(k, l) for k in range(trials) for l in range(k, trials)]

    def fold(x):
        return jnp.sum(x.reshape(occ_dev // 8, 8, LANES), axis=0)

    def tally(tile):
        where = pl.ds(pl.multiple_of(tile * LANES, LANES), LANES)
        gap = vir_energy_ref[:, where] - occ_energy_ref[...]
        x = [amps[pl.ds(k * occ_dev, occ_dev), where].astype(F32) for k in range(trials)]
        at = 0
        for k in range(trials):
            scaled = gap * x[k]
            for l in range(k, trials):
                acc[2 * at] += fold(x[k] * x[l])
                acc[2 * at + 1] += fold(scaled * x[l])
                at += 1

    def finish_tally():
        row = lax.broadcasted_iota(jnp.int32, (trials, LANES), 0)
        lane = lax.broadcasted_iota(jnp.int32, (trials, LANES), 1)
        out = jnp.zeros((trials, LANES), F32)
        for at, (k, l) in enumerate(pairs):
            for part in range(2):
                value = jnp.sum(
                    jnp.sum(acc[2 * at + part], axis=0, keepdims=True), axis=1, keepdims=True
                )
                up = (row == k) & (lane == part * trials + l)
                down = (row == l) & (lane == part * trials + k)
                out = jnp.where(up | down, value, out)
        box_ao[col, :, pl.ds(total, LANES)] = out

    for way in range(2):
        for j in range(pieces):
            hop(way, j, own, 0).start()
    dens[...] = jnp.zeros_like(dens)
    acc[...] = jnp.zeros_like(acc)
    take_amps.wait()
    for way in range(2):
        for j in range(pieces):
            contract(way, j, own)

    slots = max((n - 2) * pieces, 1)
    per = -(-tiles // slots)

    def ring_step(step, carry):
        arrived = (slot_of(0, step + 1), slot_of(1, step + 1))
        for j in range(pieces):
            for way in range(2):
                hop(way, j, arrived[way], step).wait_recv()

                @pl.when(step < n - 2)
                def _():
                    @pl.when(step >= 1)
                    def _():
                        hop(way, j, arrived[way], step - 1).wait_send()

                    hop(way, j, arrived[way], step + 1).start()

            for way in range(2):
                contract(way, j, arrived[way])

            def unit(u, c):
                tile = (step * pieces + j) * per + u

                @pl.when(tile < tiles)
                def _():
                    tally(tile)

                return c

            lax.fori_loop(0, per, unit, 0)
            if j == 0:

                @pl.when(step == n - 2)
                def _():
                    finish_tally()

        return carry

    lax.fori_loop(0, n - 1, ring_step, 0)
    give_rows = pltpu.make_async_copy(rows, rows_hbm, local_sem.at[0])
    give_rows.start()
    box_ao[col, :, pl.ds(0, total)] = jnp.concatenate([dens[b] for b in range(n)], axis=1)
    exchange(box_ao, col, m, "ao", ao_send, ao_recv)
    value = box_ao[0]
    for d in range(1, m):
        value = value + box_ao[d]
    box_occ[own] = value
    exchange(box_occ, own, n, "occ", occ_send, occ_recv)
    value = box_occ[0]
    for d in range(1, n):
        value = value + box_occ[d]
    stats_ref[...] = value
    for way in range(2):
        for j in range(pieces):
            for step in range(max(n - 3, 0), n - 1):
                hop(way, j, own, step).wait_send()
    give_rows.wait()


def apply_kernel(
    trials,
    width,
    amps_hbm,
    rows_hbm,
    occ_ref,
    occ_energy_ref,
    vir_energy_ref,
    kernel_ref,
    stats_ref,
    out_hbm,
    projected_ref,
    amps,
    rows,
    out,
    weighted,
    shift,
    in_sem,
    out_sem,
):
    occ_dev = amps.shape[0] // trials
    total = rows.shape[0]
    count = amps.shape[1] // width

    def span(c):
        return pl.ds(pl.multiple_of(c * width, width), width)

    def take(c):
        return (
            pltpu.make_async_copy(rows_hbm.at[:, span(c)], rows.at[:, span(c)], in_sem.at[0, c]),
            pltpu.make_async_copy(amps_hbm.at[:, span(c)], amps.at[:, span(c)], in_sem.at[1, c]),
        )

    def give(c):
        return pltpu.make_async_copy(out.at[:, span(c)], out_hbm.at[:, span(c)], out_sem.at[c])

    for c in range(count):
        for copy in take(c):
            copy.start()

    density = stats_ref[:, pl.ds(0, total)]
    potential = kernel_ref[...] * density
    correlation = stats_ref[:, pl.ds(total, trials)]
    gram = stats_ref[:, pl.ds(total + trials, trials)]
    lane = lax.broadcasted_iota(jnp.int32, (trials, trials), 1)
    row = lax.broadcasted_iota(jnp.int32, (trials, trials), 0)
    for l in range(trials):
        coupled = jnp.sum(density * potential[l : l + 1], axis=1, keepdims=True)
        gram = gram + jnp.where(lane == l, coupled, 0.0)
    diagonal = jnp.where(lane == row, correlation + 1e-06, 0.0)
    norm_column = jnp.sum(diagonal, axis=1, keepdims=True)
    norm_row = jnp.sum(diagonal, axis=0, keepdims=True)
    projected_ref[...] = gram / jnp.sqrt(norm_column * norm_row)
    ritz = jnp.sum(jnp.where(lane == row, gram, 0.0), axis=1, keepdims=True) / norm_column
    for k in range(trials):
        own = pl.ds(k * occ_dev, occ_dev)
        weighted[own, :] = (occ_ref[...] * potential[k : k + 1]).astype(weighted.dtype)
        shift[own, :] = jnp.broadcast_to(
            occ_energy_ref[...] + ritz[k : k + 1], (occ_dev, LANES)
        )

    def block(c, carry):
        for copy in take(c):
            copy.wait()
        coupling = jnp.dot(weighted[...], rows[:, span(c)], preferred_element_type=F32)
        for t in range(width // LANES):
            here = pl.ds(pl.multiple_of(c * width + t * LANES, LANES), LANES)
            gap = vir_energy_ref[:, here] - shift[...]
            part = coupling[:, t * LANES : (t + 1) * LANES]
            out[:, here] = (gap * amps[:, here].astype(F32) + part).astype(out.dtype)
        give(c).start()
        return carry

    lax.fori_loop(0, count, block, 0)
    for c in range(count):
        give(c).wait()


def shards(n, m, amplitudes, occ_coef, vir_coef, occ_energy, vir_energy, kernel):
    trials, occ_dev, vir_dev = amplitudes.shape
    row_dev = vir_coef.shape[0]
    total = occ_coef.shape[0]
    flat = amplitudes.reshape(trials * occ_dev, vir_dev)
    tiles = vir_dev // LANES
    parts = 4 if n <= 16 else 1
    runs = (split_tiles(0, tiles // 2, parts), split_tiles(tiles // 2, tiles, parts))
    pieces = len(runs[0])
    length = total + LANES
    occ_trans = occ_coef.T.astype(F32)
    occ_blocks = jnp.transpose(occ_coef.reshape(n, row_dev, occ_dev), (0, 2, 1)).astype(F32)
    energy_column = occ_energy[:, None]
    energy_row = vir_energy[None, :]
    vmem = pl.BlockSpec(memory_space=pltpu.VMEM)
    any_space = pl.BlockSpec(memory_space=pl.ANY)
    dma = pltpu.SemaphoreType.DMA
    matmul_flops = 2 * trials * occ_dev * vir_dev * total
    rows, stats = pl.pallas_call(
        functools.partial(gather_kernel, n, m, trials, runs),
        out_shape=(
            jax.ShapeDtypeStruct((n, row_dev, vir_dev), vir_coef.dtype),
            jax.ShapeDtypeStruct((trials, length), F32),
        ),
        in_specs=[any_space, any_space, vmem, vmem, vmem],
        out_specs=(any_space, vmem),
        scratch_shapes=[
            pltpu.VMEM((trials * occ_dev, vir_dev), amplitudes.dtype),
            pltpu.VMEM((n, row_dev, vir_dev), vir_coef.dtype),
            pltpu.VMEM((n, trials, row_dev), F32),
            pltpu.VMEM((trials * (trials + 1), 8, LANES), F32),
            pltpu.VMEM((m, trials, length), F32),
            pltpu.VMEM((n, trials, length), F32),
            dma((2,)),
            dma((2, pieces, 2)),
            dma((2, pieces, n - 1)),
            dma((m - 1,)),
            dma((m,)),
            dma((n - 1,)),
            dma((n,)),
        ],
        compiler_params=pltpu.CompilerParams(collective_id=0, has_side_effects=True),
        cost_estimate=pl.CostEstimate(
            flops=matmul_flops, bytes_accessed=flat.size * 4, transcendentals=0
        ),
    )(flat, vir_coef, occ_blocks, energy_column, energy_row)
    width = 2 * LANES if tiles % 2 == 0 else LANES
    count = vir_dev // width
    residual, projected = pl.pallas_call(
        functools.partial(apply_kernel, trials, width),
        out_shape=(
            jax.ShapeDtypeStruct(flat.shape, amplitudes.dtype),
            jax.ShapeDtypeStruct((trials, trials), F32),
        ),
        in_specs=[any_space, any_space, vmem, vmem, vmem, vmem, vmem],
        out_specs=(any_space, vmem),
        scratch_shapes=[
            pltpu.VMEM(flat.shape, amplitudes.dtype),
            pltpu.VMEM((total, vir_dev), vir_coef.dtype),
            pltpu.VMEM(flat.shape, amplitudes.dtype),
            pltpu.VMEM((trials * occ_dev, total), jnp.bfloat16),
            pltpu.VMEM((trials * occ_dev, LANES), F32),
            dma((2, count)),
            dma((count,)),
        ],
        cost_estimate=pl.CostEstimate(
            flops=matmul_flops, bytes_accessed=flat.size * 6, transcendentals=0
        ),
    )(
        flat,
        rows.reshape(total, vir_dev),
        occ_trans,
        energy_column,
        energy_row,
        kernel[None, :],
        stats,
    )
    return residual.reshape(amplitudes.shape), projected


def solution(mesh):
    placed = (P(None, "occ", "ao"), P(None, "occ"), P("occ", "ao"), P("occ"), P("ao"), P())
    return jax.shard_map(
        functools.partial(shards, mesh.shape["occ"], mesh.shape["ao"]),
        mesh=mesh,
        in_specs=placed,
        out_specs=(P(None, "occ", "ao"), P()),
        check_vma=False,
    )
```

```python
import functools

import jax
import jax.numpy as jnp
from jax import lax
from jax.experimental import pallas as pl
from jax.experimental.pallas import tpu as pltpu
from jax.sharding import PartitionSpec as P

LANES = 128
MESH = pl.DeviceIdType.MESH
F32 = jnp.float32


def split_tiles(first, last, parts):
    parts = min(parts, last - first)
    runs, at = [], first
    for j in range(parts):
        size = (last - at) // (parts - j)
        size += 1 if (last - at) % (parts - j) else 0
        runs.append((at * LANES, size * LANES))
        at += size
    return runs


def as_column(row):
    count = row.shape[1]
    here = lax.broadcasted_iota(jnp.int32, (count, count), 0)
    lane = lax.broadcasted_iota(jnp.int32, (count, count), 1)
    return jnp.sum(jnp.where(here == lane, row, 0.0), axis=1, keepdims=True)


def exchange(box, me, size, axis, send, recv):
    copies = []
    for d in range(1, size):
        copy = pltpu.make_async_remote_copy(
            src_ref=box.at[me],
            dst_ref=box.at[me],
            send_sem=send.at[d - 1],
            recv_sem=recv.at[me],
            device_id={axis: lax.rem(me + d, size)},
            device_id_type=MESH,
        )
        copy.start()
        copies.append(copy)
    for d in range(1, size):
        other = lax.rem(me + d, size)
        pltpu.make_async_remote_copy(
            src_ref=box.at[other],
            dst_ref=box.at[other],
            send_sem=send.at[d - 1],
            recv_sem=recv.at[other],
            device_id={axis: other},
            device_id_type=MESH,
        ).wait_recv()
    for copy in copies:
        copy.wait_send()


def gather_kernel(
    n,
    m,
    trials,
    runs,
    amps_hbm,
    vir_hbm,
    occ_ref,
    occ_energy_ref,
    vir_energy_ref,
    rows_hbm,
    stats_ref,
    amps,
    rows,
    dens,
    acc,
    occ_blocks,
    energy_column,
    box_ao,
    box_occ,
    local_sem,
    send_sem,
    recv_sem,
    ao_send,
    ao_recv,
    occ_send,
    occ_recv,
):
    own, col = lax.axis_index("occ"), lax.axis_index("ao")
    occ_dev = amps.shape[0] // trials
    tiles = amps.shape[1] // LANES
    total = n * rows.shape[1]
    pieces = len(runs[0])

    def place(p):
        back = p // (n // 2)
        return (1 - back) * 2 * p + back * (2 * (n - 1 - p) + 1)

    parity, half = lax.rem(own, 2), own // 2
    spot = parity * (n - 1 - half) + (1 - parity) * half
    toward = (place(lax.rem(spot + 1, n)), place(lax.rem(spot + n - 1, n)))

    take_rows = pltpu.make_async_copy(vir_hbm, rows.at[own], local_sem.at[0])
    take_rows.start()
    take_amps = pltpu.make_async_copy(amps_hbm, amps, local_sem.at[1])

    barrier = pltpu.get_barrier_semaphore()
    for d in range(1, n):
        pl.semaphore_signal(
            barrier, inc=1, device_id={"occ": lax.rem(own + d, n)}, device_id_type=MESH
        )
    for d in range(1, m):
        pl.semaphore_signal(
            barrier, inc=1, device_id={"ao": lax.rem(col + d, m)}, device_id_type=MESH
        )
    take_rows.wait()
    take_amps.start()
    pl.semaphore_wait(barrier, n + m - 2)

    def slot_of(way, age):
        if way == 0:
            return place(lax.rem(spot - age + n, n))
        return place(lax.rem(spot + age, n))

    def hop(way, j, slot, step):
        start, width = runs[way][j]
        piece = rows.at[slot, :, pl.ds(start, width)]
        return pltpu.make_async_remote_copy(
            src_ref=piece,
            dst_ref=piece,
            send_sem=send_sem.at[way, j, lax.rem(step, 2)],
            recv_sem=recv_sem.at[way, j, step],
            device_id={"occ": toward[way]},
            device_id_type=MESH,
        )

    def contract(way, j, slot):
        start, width = runs[way][j]
        half_done = lax.dot_general(
            amps[:, pl.ds(start, width)],
            rows[slot, :, pl.ds(start, width)],
            (((1,), (1,)), ((), ())),
            preferred_element_type=F32,
        )
        half_done = half_done.reshape(trials, occ_dev, rows.shape[1])
        dens[slot] += jnp.sum(half_done * occ_blocks[slot][None], axis=1)

    pairs = [(k, l) for k in range(trials) for l in range(k, trials)]

    def fold(x):
        return jnp.sum(x.reshape(occ_dev // 8, 8, LANES), axis=0)

    def tally(tile):
        where = pl.ds(pl.multiple_of(tile * LANES, LANES), LANES)
        gap = vir_energy_ref[where][None, :] - energy_column[...]
        x = [amps[pl.ds(k * occ_dev, occ_dev), where].astype(F32) for k in range(trials)]
        at = 0
        for k in range(trials):
            scaled = gap * x[k]
            for l in range(k, trials):
                acc[2 * at] += fold(x[k] * x[l])
                acc[2 * at + 1] += fold(scaled * x[l])
                at += 1

    def finish_tally():
        row = lax.broadcasted_iota(jnp.int32, (trials, LANES), 0)
        lane = lax.broadcasted_iota(jnp.int32, (trials, LANES), 1)
        out = jnp.zeros((trials, LANES), F32)
        for at, (k, l) in enumerate(pairs):
            for part in range(2):
                value = jnp.sum(
                    jnp.sum(acc[2 * at + part], axis=0, keepdims=True), axis=1, keepdims=True
                )
                up = (row == k) & (lane == part * trials + l)
                down = (row == l) & (lane == part * trials + k)
                out = jnp.where(up | down, value, out)
        box_ao[col, :, pl.ds(total, LANES)] = out

    for way in range(2):
        for j in range(pieces):
            hop(way, j, own, 0).start()
    dens[...] = jnp.zeros_like(dens)
    acc[...] = jnp.zeros_like(acc)
    occ_float = occ_ref[...].astype(F32)
    row_dev = rows.shape[1]
    for b in range(n):
        occ_blocks[b] = occ_float[:, b * row_dev : (b + 1) * row_dev]
    energy_column[...] = jnp.broadcast_to(as_column(occ_energy_ref[...]), (occ_dev, LANES))
    take_amps.wait()
    for way in range(2):
        for j in range(pieces):
            contract(way, j, own)

    slots = max((n - 2) * pieces, 1)
    per = -(-tiles // slots)

    def ring_step(step, carry):
        arrived = (slot_of(0, step + 1), slot_of(1, step + 1))
        for j in range(pieces):
            for way in range(2):
                hop(way, j, arrived[way], step).wait_recv()

                @pl.when(step < n - 2)
                def _():
                    @pl.when(step >= 1)
                    def _():
                        hop(way, j, arrived[way], step - 1).wait_send()

                    hop(way, j, arrived[way], step + 1).start()

            for way in range(2):
                contract(way, j, arrived[way])

            def unit(u, c):
                tile = (step * pieces + j) * per + u

                @pl.when(tile < tiles)
                def _():
                    tally(tile)

                return c

            lax.fori_loop(0, per, unit, 0)
            if j == 0:

                @pl.when(step == n - 2)
                def _():
                    finish_tally()

        return carry

    lax.fori_loop(0, n - 1, ring_step, 0)
    give_rows = pltpu.make_async_copy(rows, rows_hbm, local_sem.at[0])
    give_rows.start()
    box_ao[col, :, pl.ds(0, total)] = jnp.concatenate([dens[b] for b in range(n)], axis=1)
    exchange(box_ao, col, m, "ao", ao_send, ao_recv)
    value = box_ao[0]
    for d in range(1, m):
        value = value + box_ao[d]
    box_occ[own] = value
    exchange(box_occ, own, n, "occ", occ_send, occ_recv)
    value = box_occ[0]
    for d in range(1, n):
        value = value + box_occ[d]
    stats_ref[...] = value
    for way in range(2):
        for j in range(pieces):
            for step in range(max(n - 3, 0), n - 1):
                hop(way, j, own, step).wait_send()
    give_rows.wait()


def apply_kernel(
    trials,
    width,
    amps_hbm,
    rows_hbm,
    occ_ref,
    occ_energy_ref,
    vir_energy_ref,
    kernel_ref,
    stats_ref,
    out_hbm,
    projected_ref,
    amps,
    rows,
    out,
    weighted,
    shift,
    in_sem,
    out_sem,
):
    occ_dev = amps.shape[0] // trials
    total = rows.shape[0]
    count = amps.shape[1] // width

    def span(c):
        return pl.ds(pl.multiple_of(c * width, width), width)

    def take(c):
        return (
            pltpu.make_async_copy(rows_hbm.at[:, span(c)], rows.at[:, span(c)], in_sem.at[0, c]),
            pltpu.make_async_copy(amps_hbm.at[:, span(c)], amps.at[:, span(c)], in_sem.at[1, c]),
        )

    def give(c):
        return pltpu.make_async_copy(out.at[:, span(c)], out_hbm.at[:, span(c)], out_sem.at[c])

    ahead = min(6, count)
    for c in range(ahead):
        for copy in take(c):
            copy.start()

    density = stats_ref[:, pl.ds(0, total)]
    potential = kernel_ref[...] * density
    correlation = stats_ref[:, pl.ds(total, trials)]
    gram = stats_ref[:, pl.ds(total + trials, trials)]
    lane = lax.broadcasted_iota(jnp.int32, (trials, trials), 1)
    row = lax.broadcasted_iota(jnp.int32, (trials, trials), 0)
    for l in range(trials):
        coupled = jnp.sum(density * potential[l : l + 1], axis=1, keepdims=True)
        gram = gram + jnp.where(lane == l, coupled, 0.0)
    diagonal = jnp.where(lane == row, correlation + 1e-06, 0.0)
    norm_column = jnp.sum(diagonal, axis=1, keepdims=True)
    norm_row = jnp.sum(diagonal, axis=0, keepdims=True)
    projected_ref[...] = gram / jnp.sqrt(norm_column * norm_row)
    ritz = jnp.sum(jnp.where(lane == row, gram, 0.0), axis=1, keepdims=True) / norm_column
    occ_float = occ_ref[...].astype(F32)
    energy_column = as_column(occ_energy_ref[...])
    for k in range(trials):
        own = pl.ds(k * occ_dev, occ_dev)
        weighted[own, :] = (occ_float * potential[k : k + 1]).astype(weighted.dtype)
        shift[own, :] = jnp.broadcast_to(energy_column + ritz[k : k + 1], (occ_dev, LANES))

    def blocks(first, size):
        for c in range(size):
            later = first + c + ahead

            @pl.when(later < count)
            def _():
                for copy in take(later):
                    copy.start()

        for c in range(size):
            for copy in take(first + c):
                copy.wait()
        for c in range(size):
            at = (first + c) * width
            coupling = jnp.dot(
                weighted[...], rows[:, span(first + c)], preferred_element_type=F32
            )
            for t in range(width // LANES):
                here = pl.ds(pl.multiple_of(at + t * LANES, LANES), LANES)
                gap = vir_energy_ref[here][None, :] - shift[...]
                part = coupling[:, t * LANES : (t + 1) * LANES]
                out[:, here] = (gap * amps[:, here].astype(F32) + part).astype(out.dtype)
        for c in range(size):
            give(first + c).start()

    group = 3
    lead = count % group
    if lead:
        blocks(0, lead)

    def turn(g, carry):
        blocks(lead + g * group, group)
        return carry

    lax.fori_loop(0, count // group, turn, 0)
    for c in range(count):
        give(c).wait()


def shards(n, m, amplitudes, occ_coef, vir_coef, occ_energy, vir_energy, kernel):
    trials, occ_dev, vir_dev = amplitudes.shape
    row_dev = vir_coef.shape[0]
    total = occ_coef.shape[0]
    flat = amplitudes.reshape(trials * occ_dev, vir_dev)
    tiles = vir_dev // LANES
    parts = 4 if n <= 16 else 1
    runs = (split_tiles(0, tiles // 2, parts), split_tiles(tiles // 2, tiles, parts))
    pieces = len(runs[0])
    length = total + LANES
    occ_trans = occ_coef.T
    energy_row = occ_energy[None, :]
    vmem = pl.BlockSpec(memory_space=pltpu.VMEM)
    any_space = pl.BlockSpec(memory_space=pl.ANY)
    dma = pltpu.SemaphoreType.DMA
    matmul_flops = 2 * trials * occ_dev * vir_dev * total
    rows, stats = pl.pallas_call(
        functools.partial(gather_kernel, n, m, trials, runs),
        out_shape=(
            jax.ShapeDtypeStruct((n, row_dev, vir_dev), vir_coef.dtype),
            jax.ShapeDtypeStruct((trials, length), F32),
        ),
        in_specs=[any_space, any_space, vmem, vmem, vmem],
        out_specs=(any_space, vmem),
        scratch_shapes=[
            pltpu.VMEM((trials * occ_dev, vir_dev), amplitudes.dtype),
            pltpu.VMEM((n, row_dev, vir_dev), vir_coef.dtype),
            pltpu.VMEM((n, trials, row_dev), F32),
            pltpu.VMEM((trials * (trials + 1), 8, LANES), F32),
            pltpu.VMEM((n, occ_dev, row_dev), F32),
            pltpu.VMEM((occ_dev, LANES), F32),
            pltpu.VMEM((m, trials, length), F32),
            pltpu.VMEM((n, trials, length), F32),
            dma((2,)),
            dma((2, pieces, 2)),
            dma((2, pieces, n - 1)),
            dma((m - 1,)),
            dma((m,)),
            dma((n - 1,)),
            dma((n,)),
        ],
        compiler_params=pltpu.CompilerParams(collective_id=0, has_side_effects=True),
        cost_estimate=pl.CostEstimate(
            flops=matmul_flops, bytes_accessed=flat.size * 4, transcendentals=0
        ),
    )(flat, vir_coef, occ_trans, energy_row, vir_energy)
    width = 2 * LANES if tiles % 2 == 0 else LANES
    count = vir_dev // width
    residual, projected = pl.pallas_call(
        functools.partial(apply_kernel, trials, width),
        out_shape=(
            jax.ShapeDtypeStruct(flat.shape, amplitudes.dtype),
            jax.ShapeDtypeStruct((trials, trials), F32),
        ),
        in_specs=[any_space, any_space, vmem, vmem, vmem, vmem, vmem],
        out_specs=(any_space, vmem),
        scratch_shapes=[
            pltpu.VMEM(flat.shape, amplitudes.dtype),
            pltpu.VMEM((total, vir_dev), vir_coef.dtype),
            pltpu.VMEM(flat.shape, amplitudes.dtype),
            pltpu.VMEM((trials * occ_dev, total), jnp.bfloat16),
            pltpu.VMEM((trials * occ_dev, LANES), F32),
            dma((2, count)),
            dma((count,)),
        ],
        cost_estimate=pl.CostEstimate(
            flops=matmul_flops, bytes_accessed=flat.size * 6, transcendentals=0
        ),
    )(
        flat,
        rows.reshape(total, vir_dev),
        occ_trans,
        energy_row,
        vir_energy,
        kernel[None, :],
        stats,
    )
    return residual.reshape(amplitudes.shape), projected


def solution(mesh):
    placed = (P(None, "occ", "ao"), P(None, "occ"), P("occ", "ao"), P("occ"), P("ao"), P())
    return jax.shard_map(
        functools.partial(shards, mesh.shape["occ"], mesh.shape["ao"]),
        mesh=mesh,
        in_specs=placed,
        out_specs=(P(None, "occ", "ao"), P()),
        check_vma=False,
    )
```

```python
import functools

import jax
import jax.numpy as jnp
from jax import lax
from jax.experimental import pallas as pl
from jax.experimental.pallas import tpu as pltpu
from jax.sharding import PartitionSpec as P

LANES = 128
MESH = pl.DeviceIdType.MESH
F32 = jnp.float32


def split_tiles(first, last, parts):
    parts = min(parts, last - first)
    runs, at = [], first
    for j in range(parts):
        size = (last - at) // (parts - j)
        size += 1 if (last - at) % (parts - j) else 0
        runs.append((at * LANES, size * LANES))
        at += size
    return runs


def as_column(row):
    count = row.shape[1]
    here = lax.broadcasted_iota(jnp.int32, (count, count), 0)
    lane = lax.broadcasted_iota(jnp.int32, (count, count), 1)
    return jnp.sum(jnp.where(here == lane, row, 0.0), axis=1, keepdims=True)


def exchange(box, me, size, axis, send, recv):
    copies = []
    for d in range(1, size):
        copy = pltpu.make_async_remote_copy(
            src_ref=box.at[me],
            dst_ref=box.at[me],
            send_sem=send.at[d - 1],
            recv_sem=recv.at[me],
            device_id={axis: lax.rem(me + d, size)},
            device_id_type=MESH,
        )
        copy.start()
        copies.append(copy)
    for d in range(1, size):
        other = lax.rem(me + d, size)
        pltpu.make_async_remote_copy(
            src_ref=box.at[other],
            dst_ref=box.at[other],
            send_sem=send.at[d - 1],
            recv_sem=recv.at[other],
            device_id={axis: other},
            device_id_type=MESH,
        ).wait_recv()
    for copy in copies:
        copy.wait_send()


def gather_kernel(
    n,
    m,
    trials,
    runs,
    amps_hbm,
    vir_hbm,
    occ_ref,
    occ_energy_ref,
    vir_energy_ref,
    rows_hbm,
    stats_ref,
    amps,
    rows,
    dens,
    acc,
    occ_blocks,
    energy_column,
    box_ao,
    box_occ,
    local_sem,
    send_sem,
    recv_sem,
    ao_send,
    ao_recv,
    occ_send,
    occ_recv,
):
    own, col = lax.axis_index("occ"), lax.axis_index("ao")
    occ_dev = amps.shape[0] // trials
    tiles = amps.shape[1] // LANES
    total = n * rows.shape[1]
    pieces = len(runs[0])

    def place(p):
        back = p // (n // 2)
        return (1 - back) * 2 * p + back * (2 * (n - 1 - p) + 1)

    parity, half = lax.rem(own, 2), own // 2
    spot = parity * (n - 1 - half) + (1 - parity) * half
    toward = (place(lax.rem(spot + 1, n)), place(lax.rem(spot + n - 1, n)))

    take_rows = pltpu.make_async_copy(vir_hbm, rows.at[own], local_sem.at[0])
    take_rows.start()
    take_amps = pltpu.make_async_copy(amps_hbm, amps, local_sem.at[1])

    barrier = pltpu.get_barrier_semaphore()
    for d in range(1, n):
        pl.semaphore_signal(
            barrier, inc=1, device_id={"occ": lax.rem(own + d, n)}, device_id_type=MESH
        )
    for d in range(1, m):
        pl.semaphore_signal(
            barrier, inc=1, device_id={"ao": lax.rem(col + d, m)}, device_id_type=MESH
        )
    take_rows.wait()
    take_amps.start()
    pl.semaphore_wait(barrier, n + m - 2)

    def slot_of(way, age):
        if way == 0:
            return place(lax.rem(spot - age + n, n))
        return place(lax.rem(spot + age, n))

    def hop(way, j, slot, step):
        start, width = runs[way][j]
        piece = rows.at[slot, :, pl.ds(start, width)]
        return pltpu.make_async_remote_copy(
            src_ref=piece,
            dst_ref=piece,
            send_sem=send_sem.at[way, j, lax.rem(step, 2)],
            recv_sem=recv_sem.at[way, j, step],
            device_id={"occ": toward[way]},
            device_id_type=MESH,
        )

    def contract(way, j, slot):
        start, width = runs[way][j]
        half_done = lax.dot_general(
            amps[:, pl.ds(start, width)],
            rows[slot, :, pl.ds(start, width)],
            (((1,), (1,)), ((), ())),
            preferred_element_type=F32,
        )
        half_done = half_done.reshape(trials, occ_dev, rows.shape[1])
        dens[slot] += jnp.sum(half_done * occ_blocks[slot][None], axis=1)

    pairs = [(k, l) for k in range(trials) for l in range(k, trials)]

    def fold(x):
        return jnp.sum(x.reshape(occ_dev // 8, 8, LANES), axis=0)

    def tally(tile):
        where = pl.ds(pl.multiple_of(tile * LANES, LANES), LANES)
        gap = vir_energy_ref[where][None, :] - energy_column[...]
        x = [amps[pl.ds(k * occ_dev, occ_dev), where].astype(F32) for k in range(trials)]
        at = 0
        for k in range(trials):
            scaled = gap * x[k]
            for l in range(k, trials):
                acc[2 * at] += fold(x[k] * x[l])
                acc[2 * at + 1] += fold(scaled * x[l])
                at += 1

    def finish_tally():
        row = lax.broadcasted_iota(jnp.int32, (trials, LANES), 0)
        lane = lax.broadcasted_iota(jnp.int32, (trials, LANES), 1)
        out = jnp.zeros((trials, LANES), F32)
        for at, (k, l) in enumerate(pairs):
            for part in range(2):
                value = jnp.sum(
                    jnp.sum(acc[2 * at + part], axis=0, keepdims=True), axis=1, keepdims=True
                )
                up = (row == k) & (lane == part * trials + l)
                down = (row == l) & (lane == part * trials + k)
                out = jnp.where(up | down, value, out)
        box_ao[col, :, pl.ds(total, LANES)] = out

    for way in range(2):
        for j in range(pieces):
            hop(way, j, own, 0).start()
    dens[...] = jnp.zeros_like(dens)
    acc[...] = jnp.zeros_like(acc)
    occ_float = occ_ref[...].astype(F32)
    row_dev = rows.shape[1]
    for b in range(n):
        occ_blocks[b] = occ_float[:, b * row_dev : (b + 1) * row_dev]
    energy_column[...] = jnp.broadcast_to(as_column(occ_energy_ref[...]), (occ_dev, LANES))
    take_amps.wait()
    for way in range(2):
        for j in range(pieces):
            contract(way, j, own)

    slots = max((n - 2) * pieces, 1)
    per = -(-tiles // slots)

    def ring_step(step, carry):
        arrived = (slot_of(0, step + 1), slot_of(1, step + 1))
        for j in range(pieces):
            for way in range(2):
                hop(way, j, arrived[way], step).wait_recv()

                @pl.when(step < n - 2)
                def _():
                    @pl.when(step >= 1)
                    def _():
                        hop(way, j, arrived[way], step - 1).wait_send()

                    hop(way, j, arrived[way], step + 1).start()

            for way in range(2):
                contract(way, j, arrived[way])

            def unit(u, c):
                tile = (step * pieces + j) * per + u

                @pl.when(tile < tiles)
                def _():
                    tally(tile)

                return c

            lax.fori_loop(0, per, unit, 0)
            if j == 0:

                @pl.when(step == n - 2)
                def _():
                    finish_tally()

        return carry

    lax.fori_loop(0, n - 1, ring_step, 0)
    give_rows = pltpu.make_async_copy(rows, rows_hbm, local_sem.at[0])
    give_rows.start()
    box_ao[col, :, pl.ds(0, total)] = jnp.concatenate([dens[b] for b in range(n)], axis=1)
    exchange(box_ao, col, m, "ao", ao_send, ao_recv)
    value = box_ao[0]
    for d in range(1, m):
        value = value + box_ao[d]
    box_occ[own] = value
    exchange(box_occ, own, n, "occ", occ_send, occ_recv)
    value = box_occ[0]
    for d in range(1, n):
        value = value + box_occ[d]
    stats_ref[...] = value
    for way in range(2):
        for j in range(pieces):
            for step in range(max(n - 3, 0), n - 1):
                hop(way, j, own, step).wait_send()
    give_rows.wait()


def apply_kernel(
    trials,
    width,
    amps_hbm,
    rows_hbm,
    occ_ref,
    occ_energy_ref,
    vir_energy_ref,
    kernel_ref,
    stats_ref,
    out_hbm,
    projected_ref,
    amps,
    rows,
    out,
    weighted,
    shift,
    in_sem,
    out_sem,
):
    occ_dev = amps.shape[0] // trials
    total = rows.shape[0]
    count = amps.shape[1] // width

    group = 3
    lead = count % group
    turns = count // group

    def span(c, size=1):
        return pl.ds(pl.multiple_of(c * width, width), size * width)

    def take(first, size, sem):
        here = span(first, size)
        return (
            pltpu.make_async_copy(rows_hbm.at[:, here], rows.at[:, here], in_sem.at[0, sem]),
            pltpu.make_async_copy(amps_hbm.at[:, here], amps.at[:, here], in_sem.at[1, sem]),
        )

    def give(first, size, sem):
        here = span(first, size)
        return pltpu.make_async_copy(out.at[:, here], out_hbm.at[:, here], out_sem.at[sem])

    def take_turn(g):
        return take(lead + g * group, group, g)

    ahead = min(3, turns)
    if lead:
        for copy in take(0, lead, turns):
            copy.start()
    for g in range(ahead):
        for copy in take_turn(g):
            copy.start()

    density = stats_ref[:, pl.ds(0, total)]
    potential = kernel_ref[...] * density
    correlation = stats_ref[:, pl.ds(total, trials)]
    gram = stats_ref[:, pl.ds(total + trials, trials)]
    lane = lax.broadcasted_iota(jnp.int32, (trials, trials), 1)
    row = lax.broadcasted_iota(jnp.int32, (trials, trials), 0)
    for l in range(trials):
        coupled = jnp.sum(density * potential[l : l + 1], axis=1, keepdims=True)
        gram = gram + jnp.where(lane == l, coupled, 0.0)
    diagonal = jnp.where(lane == row, correlation + 1e-06, 0.0)
    norm_column = jnp.sum(diagonal, axis=1, keepdims=True)
    norm_row = jnp.sum(diagonal, axis=0, keepdims=True)
    projected_ref[...] = gram / jnp.sqrt(norm_column * norm_row)
    ritz = jnp.sum(jnp.where(lane == row, gram, 0.0), axis=1, keepdims=True) / norm_column
    occ_float = occ_ref[...].astype(F32)
    energy_column = as_column(occ_energy_ref[...])
    for k in range(trials):
        own = pl.ds(k * occ_dev, occ_dev)
        weighted[own, :] = (occ_float * potential[k : k + 1]).astype(weighted.dtype)
        shift[own, :] = jnp.broadcast_to(energy_column + ritz[k : k + 1], (occ_dev, LANES))

    def blocks(first, size):
        for c in range(size):
            at = (first + c) * width
            coupling = jnp.dot(
                weighted[...], rows[:, span(first + c)], preferred_element_type=F32
            )
            for t in range(width // LANES):
                here = pl.ds(pl.multiple_of(at + t * LANES, LANES), LANES)
                gap = vir_energy_ref[here][None, :] - shift[...]
                part = coupling[:, t * LANES : (t + 1) * LANES]
                out[:, here] = (gap * amps[:, here].astype(F32) + part).astype(out.dtype)

    if lead:
        for copy in take(0, lead, turns):
            copy.wait()
        blocks(0, lead)
        give(0, lead, turns).start()

    def turn(g, carry):
        @pl.when(g + ahead < turns)
        def _():
            for copy in take_turn(g + ahead):
                copy.start()

        for copy in take_turn(g):
            copy.wait()
        blocks(lead + g * group, group)
        give(lead + g * group, group, g).start()
        return carry

    lax.fori_loop(0, turns, turn, 0)
    if lead:
        give(0, lead, turns).wait()
    for g in range(turns):
        give(lead + g * group, group, g).wait()


def shards(n, m, amplitudes, occ_coef, vir_coef, occ_energy, vir_energy, kernel):
    trials, occ_dev, vir_dev = amplitudes.shape
    row_dev = vir_coef.shape[0]
    total = occ_coef.shape[0]
    flat = amplitudes.reshape(trials * occ_dev, vir_dev)
    tiles = vir_dev // LANES
    parts = 4 if n <= 16 else 1
    runs = (split_tiles(0, tiles // 2, parts), split_tiles(tiles // 2, tiles, parts))
    pieces = len(runs[0])
    length = total + LANES
    occ_trans = occ_coef.T
    energy_row = occ_energy[None, :]
    vmem = pl.BlockSpec(memory_space=pltpu.VMEM)
    any_space = pl.BlockSpec(memory_space=pl.ANY)
    dma = pltpu.SemaphoreType.DMA
    matmul_flops = 2 * trials * occ_dev * vir_dev * total
    rows, stats = pl.pallas_call(
        functools.partial(gather_kernel, n, m, trials, runs),
        out_shape=(
            jax.ShapeDtypeStruct((n, row_dev, vir_dev), vir_coef.dtype),
            jax.ShapeDtypeStruct((trials, length), F32),
        ),
        in_specs=[any_space, any_space, vmem, vmem, vmem],
        out_specs=(any_space, vmem),
        scratch_shapes=[
            pltpu.VMEM((trials * occ_dev, vir_dev), amplitudes.dtype),
            pltpu.VMEM((n, row_dev, vir_dev), vir_coef.dtype),
            pltpu.VMEM((n, trials, row_dev), F32),
            pltpu.VMEM((trials * (trials + 1), 8, LANES), F32),
            pltpu.VMEM((n, occ_dev, row_dev), F32),
            pltpu.VMEM((occ_dev, LANES), F32),
            pltpu.VMEM((m, trials, length), F32),
            pltpu.VMEM((n, trials, length), F32),
            dma((2,)),
            dma((2, pieces, 2)),
            dma((2, pieces, n - 1)),
            dma((m - 1,)),
            dma((m,)),
            dma((n - 1,)),
            dma((n,)),
        ],
        compiler_params=pltpu.CompilerParams(collective_id=0, has_side_effects=True),
        cost_estimate=pl.CostEstimate(
            flops=matmul_flops, bytes_accessed=flat.size * 4, transcendentals=0
        ),
    )(flat, vir_coef, occ_trans, energy_row, vir_energy)
    width = 2 * LANES if tiles % 2 == 0 else LANES
    count = vir_dev // width
    residual, projected = pl.pallas_call(
        functools.partial(apply_kernel, trials, width),
        out_shape=(
            jax.ShapeDtypeStruct(flat.shape, amplitudes.dtype),
            jax.ShapeDtypeStruct((trials, trials), F32),
        ),
        in_specs=[any_space, any_space, vmem, vmem, vmem, vmem, vmem],
        out_specs=(any_space, vmem),
        scratch_shapes=[
            pltpu.VMEM(flat.shape, amplitudes.dtype),
            pltpu.VMEM((total, vir_dev), vir_coef.dtype),
            pltpu.VMEM(flat.shape, amplitudes.dtype),
            pltpu.VMEM((trials * occ_dev, total), jnp.bfloat16),
            pltpu.VMEM((trials * occ_dev, LANES), F32),
            dma((2, count // 3 + 1)),
            dma((count // 3 + 1,)),
        ],
        cost_estimate=pl.CostEstimate(
            flops=matmul_flops, bytes_accessed=flat.size * 6, transcendentals=0
        ),
    )(
        flat,
        rows.reshape(total, vir_dev),
        occ_trans,
        energy_row,
        vir_energy,
        kernel[None, :],
        stats,
    )
    return residual.reshape(amplitudes.shape), projected


def solution(mesh):
    placed = (P(None, "occ", "ao"), P(None, "occ"), P("occ", "ao"), P("occ"), P("ao"), P())
    return jax.shard_map(
        functools.partial(shards, mesh.shape["occ"], mesh.shape["ao"]),
        mesh=mesh,
        in_specs=placed,
        out_specs=(P(None, "occ", "ao"), P()),
        check_vma=False,
    )
```
